32 devices in a mesh: row: 4 (over y, x), col: 8 (over z, core).
Axes of the slice: x: 2, y: 2, z: 4, core: 2. Of those that a mesh axis runs over, the one named last changes fastest.
Arguments:
- tiles: bfloat16 [1024, 256, 256], P(('row', 'col')), as said below
- tile_row: int32 [1024], P(('row', 'col')), may hold values from 0 to 31, as said below
- tile_col: int32 [1024], P(('row', 'col')), may hold values from 0 to 31, as said below
- label_class: int32 [8192], P(('row', 'col')), may hold values from -1 to 127, as said below
Outputs:
- scores: float32 [8192, 128], P(('row', 'col'))
- residual: float32 [8192, 128], P(('row', 'col'))
The draws below stay inside these ranges and needn't reach their ends.
Inputs may be any that keep to these rules, and one draw needn't show every extreme that they name: `tiles`: Nonnegative. The tile of blocks (j, i) is the transpose of the tile of blocks (i, j); a tile on the diagonal is symmetric. No pair of blocks appears twice; the pair (j, i) is stored whenever (i, j) is. The device with row index r and col index c holds 32 tiles, all with tile_row // 8 == r and tile_col % 8 == c. `tile_col`: see tile_row. `label_class`: exactly 1024 nodes are labeled, and every class labels at least one node.
All inputs are finite; a program needn't handle non-finite values.
Results may differ from the reference program's by a relative error of at most 0.00062.
Values may be sent and summed in bfloat16 or wider, within the bound.
A program may use at most 64 MiB of HBM per device.

```python
import jax
import jax.numpy as jnp
from jax import lax

TILE = 256
CLASSES = 128
ITERS = 3
BLOCKS = 32
TILES_DEV = 32
NODES = 8192
N_COL = 8


def tile_pattern(key):
    pair_count = (TILES_DEV - 2) // 2
    shuffled = jax.random.permutation(jax.random.fold_in(key, 11), BLOCKS // 2 - 1) + 1
    chosen = shuffled[:pair_count].astype(jnp.int32)
    offsets = jnp.concatenate([jnp.array([0, BLOCKS // 2], jnp.int32), chosen, BLOCKS - chosen]).astype(jnp.int32)
    device = jnp.arange(BLOCKS, dtype=jnp.int32)[:, None]
    row_index = device // N_COL
    col_index = device % N_COL
    col_part = (col_index - offsets[None, :]) % N_COL
    rows = row_index * N_COL + col_part
    cols = (rows + offsets[None, :]) % BLOCKS
    return (rows.reshape(-1).astype(jnp.int32), cols.reshape(-1).astype(jnp.int32))


def draw_tile_row(key, part):
    return tile_pattern(key)[0]


def draw_tile_col(key, part):
    return tile_pattern(key)[1]


def draw_tiles(key, part):
    rows, cols = tile_pattern(key)
    smaller = jnp.minimum(rows, cols)
    larger = jnp.maximum(rows, cols)
    pair_id = smaller * BLOCKS + larger
    scale_value = 400.0 * CLASSES / (TILES_DEV * TILE)

    def one_tile(element):
        pair_value, transposed, on_diagonal = element
        pair_key = jax.random.fold_in(jax.random.fold_in(key, 23), pair_value)
        first_key, second_key = jax.random.split(pair_key)
        entries = jnp.exp(-6.0 * jax.random.uniform(first_key, (TILE, TILE), jnp.float32))
        factor = jnp.exp(jnp.log(0.01) * jax.random.uniform(second_key, (), jnp.float32))
        entries = entries * factor
        entries = jnp.where(on_diagonal, 0.5 * (entries + entries.T), jnp.where(transposed, entries.T, entries))
        return (entries * scale_value).astype(jnp.bfloat16)
    return lax.map(one_tile, (pair_id, rows > cols, rows == cols))


def draw_label_class(key, part):
    shuffled = jax.random.permutation(jax.random.fold_in(key, 5), NODES)
    random_class = jax.random.randint(jax.random.fold_in(key, 6), (NODES,), 0, CLASSES)
    ranking = jnp.arange(NODES, dtype=jnp.int32)
    assigned = jnp.where(ranking < CLASSES, ranking, random_class)
    assigned = jnp.where(ranking < NODES // 8, assigned, -1).astype(jnp.int32)
    return jnp.zeros((NODES,), jnp.int32).at[shuffled].set(assigned)


def setup_inputs(seed: int = 0) -> dict:
    splits = jax.random.split(jax.random.key(seed), 5)
    tiles = draw_tiles(jax.random.fold_in(splits[4], 71), 0)
    tile_row = draw_tile_row(jax.random.fold_in(splits[4], 71), 0)
    tile_col = draw_tile_col(jax.random.fold_in(splits[4], 71), 0)
    label_class = draw_label_class(jax.random.fold_in(splits[4], 71), 0)
    return {"tiles": tiles, "tile_row": tile_row, "tile_col": tile_col, "label_class": label_class}


def weight_apply(tiles, tile_row, tile_col, vector_half):
    source = vector_half.reshape(BLOCKS, TILE, CLASSES).astype(jnp.float32)
    grouped = tiles.reshape(BLOCKS, TILES_DEV, TILE, TILE)
    grouped_rows = tile_row.reshape(BLOCKS, TILES_DEV).astype(jnp.int32)
    grouped_cols = tile_col.reshape(BLOCKS, TILES_DEV).astype(jnp.int32)

    def one_group(running, element):
        tile_block, block_row, block_col = element
        products = jnp.einsum("tab,tbk->tak", tile_block.astype(jnp.float32), source[block_col], precision=lax.Precision.HIGHEST)
        return running.at[block_row].add(products), None

    start = jnp.zeros((BLOCKS, TILE, CLASSES), jnp.float32)
    running, _ = lax.scan(one_group, start, (grouped, grouped_rows, grouped_cols))
    return running.reshape(NODES, CLASSES)


def reference(tiles, tile_row, tile_col, label_class):
    row_sums = jnp.sum(tiles.astype(jnp.float32), axis=2)
    degree = jax.ops.segment_sum(row_sums, tile_row.astype(jnp.int32), num_segments=BLOCKS).reshape(NODES)
    unlabeled = label_class < 0
    onehot = (label_class[:, None] == jnp.arange(CLASSES, dtype=jnp.int32)[None, :]).astype(jnp.bfloat16)
    rhs = jnp.where(unlabeled[:, None], weight_apply(tiles, tile_row, tile_col, onehot), jnp.float32(0.0))

    def operator(direction):
        mixed = weight_apply(tiles, tile_row, tile_col, direction.astype(jnp.bfloat16))
        return jnp.where(unlabeled[:, None], degree[:, None] * direction - mixed, direction)

    solution = jnp.zeros((NODES, CLASSES), jnp.float32)
    residual = rhs
    direction = rhs
    norm_now = jnp.sum(residual * residual, axis=0)
    for iteration in range(ITERS):
        image = operator(direction)
        alpha = norm_now / jnp.sum(direction * image, axis=0)
        solution = solution + alpha * direction
        residual = residual - alpha * image
        norm_next = jnp.sum(residual * residual, axis=0)
        direction = residual + (norm_next / norm_now) * direction
        norm_now = norm_next
    return 8.0 * CLASSES * solution, residual
```

```python
import functools

import jax
import jax.numpy as jnp
from jax import lax
from jax.experimental import pallas as pl
from jax.experimental.pallas import tpu as pltpu
from jax.sharding import PartitionSpec as P

CLASSES = 128
ITERS = 3
PAD = 16
DEG = 8
UNROLL = 32
PARTS = 4


def each(count, body, unroll):
    if unroll:
        for n in range(count):
            body(n)
    else:
        def step(n, carry):
            body(n)
            return carry
        lax.fori_loop(0, count, step, 0)


def flip(index, mask):
    bit = 1
    result = index
    while bit <= mask:
        if mask & bit:
            result = result + bit * (1 - 2 * lax.rem(lax.div(index, bit), 2))
        bit *= 2
    return result


def kernel(
    R, C, pos, label_ref, tiles_hbm, x_out, r_out,
    tiles, lab, ag0, ag, acc0, acc, rs0, rs, st_ag, st_row, st_rs,
    degree, unlabeled, direction, image,
    tile_sem, lab_send, lab_recv, ag_send, ag_recv, st_send, st_recv,
    str_send, str_recv, rs_send, rs_recv,
):
    T, B = tiles_hbm.shape[0], tiles_hbm.shape[1]
    Z = C // 2
    K = CLASSES
    unroll = R * C <= UNROLL
    row, col = lax.axis_index("row"), lax.axis_index("col")
    core = lax.rem(col, 2)
    peer = col + 1 - 2 * core
    pow2_z = Z & (Z - 1) == 0
    pow2_r = R & (R - 1) == 0
    assert pow2_z and pow2_r

    def col_partner(m):
        return flip(col, m)

    def row_partner(m):
        return flip(row, m)

    step = -(-T // PARTS)
    tile_copies = []
    for p in range(PARTS):
        lo, hi = p * step, min(T, (p + 1) * step)
        if lo < hi:
            cp = pltpu.make_async_copy(
                tiles_hbm.at[pl.ds(lo, hi - lo)], tiles.at[pl.ds(lo, hi - lo)], tile_sem.at[p]
            )
            cp.start()
            tile_copies.append(cp)
    if tiles.shape[0] > T:
        tiles[T] = jnp.zeros((B, B), jnp.bfloat16)

    barrier = pltpu.get_barrier_semaphore()
    for m in range(1, C):
        pl.semaphore_signal(
            barrier, inc=1, device_id={"col": col_partner(m)}, device_id_type=pl.DeviceIdType.MESH
        )
    for m in range(1, R):
        pl.semaphore_signal(
            barrier, inc=1, device_id={"row": row_partner(m)}, device_id_type=pl.DeviceIdType.MESH
        )
    mine = label_ref[...]
    lab[col] = jnp.broadcast_to(mine, (8, B))
    pl.semaphore_wait(barrier, C - 1 + R - 1)

    sent = []

    def send(src, dst, send_sem, recv_sem, where):
        cp = pltpu.make_async_remote_copy(
            src_ref=src, dst_ref=dst, send_sem=send_sem, recv_sem=recv_sem,
            device_id=where, device_id_type=pl.DeviceIdType.MESH,
        )
        cp.start()
        sent.append(cp)

    def arrive(dst, recv_sem):
        pltpu.make_async_remote_copy(
            src_ref=dst, dst_ref=dst, send_sem=tile_sem.at[0], recv_sem=recv_sem,
            device_id={"col": peer}, device_id_type=pl.DeviceIdType.MESH,
        ).wait_recv()

    def tile_at(source, k):
        return tiles[pos[source * R + k]]

    def scatter(stage, total, slots, k_body):
        for m in range(R - 1, 0, -1):
            k = row_partner(m)
            k_body(k)
            send(total.at[k], slots.at[m - 1], rs_send.at[stage, m], rs_recv.at[stage, m],
                 {"row": k})
        k_body(row)
        result = total[row]
        for m in range(1, R):
            arrive(slots.at[m - 1], rs_recv.at[stage, m])
            result = result + slots[m - 1]
        return result

    def stats_start(s, rows):
        padded = jnp.concatenate(rows + [jnp.zeros((8 - len(rows), K), jnp.float32)], axis=0)
        st_ag[s, col] = padded
        for m in range(1, C):
            send(st_ag.at[s, col], st_ag.at[s, col], st_send.at[s, m], st_recv.at[s, col],
                 {"col": col_partner(m)})

    def stats_middle(s):
        for m in range(1, C):
            c = col_partner(m)
            arrive(st_ag.at[s, c], st_recv.at[s, c])
        st_row[s] = jnp.sum(st_ag[s], axis=0)
        for m in range(1, R):
            send(st_row.at[s], st_rs.at[s, row], str_send.at[s, m], str_recv.at[s, row],
                 {"row": row_partner(m)})
        st_rs[s, row] = st_row[s]

    def stats_end(s):
        for m in range(1, R):
            k = row_partner(m)
            arrive(st_rs.at[s, k], str_recv.at[s, k])
        return jnp.sum(st_rs[s], axis=0)

    for m in range(1, C):
        send(lab.at[col], lab.at[col], lab_send.at[m], lab_recv.at[col], {"col": col_partner(m)})
    class_axis = lax.broadcasted_iota(jnp.int32, (K, B), 0)
    ones = jnp.ones((PAD, B), jnp.bfloat16)

    def encode(c):
        hot = jnp.where(lab[c][0:1] == class_axis, 1.0, 0.0).astype(jnp.bfloat16)
        ag0[c] = jnp.concatenate([hot, ones], axis=0)

    encode(col)
    unlabeled[...] = jnp.where(jnp.broadcast_to(mine, (K, B)) < 0, 1.0, 0.0).T
    for m in range(1, C):
        c = col_partner(m)
        arrive(lab.at[c], lab_recv.at[c])
        encode(c)
    for cp in tile_copies:
        cp.wait()

    def first_products(k):
        if unroll:
            value = jnp.zeros((K + PAD, B), jnp.float32)
            for c in range(C):
                value = value + jnp.dot(ag0[c], tile_at(c, k), preferred_element_type=jnp.float32)
        else:
            value = lax.fori_loop(
                0, C,
                lambda c, v: v + jnp.dot(ag0[c], tile_at(c, k), preferred_element_type=jnp.float32),
                jnp.zeros((K + PAD, B), jnp.float32),
            )
        acc0[k] = value[: K + DEG]

    total = scatter(0, acc0, rs0, first_products)
    free = unlabeled[...] > 0.0
    degree[...] = jnp.broadcast_to(total[K : K + 1], (K, B)).T
    rhs = jnp.where(free, total[:K].T, 0.0)

    def inner(a, b):
        return jnp.sum(a * b, axis=0, keepdims=True)

    def operator(stage, v, first_norm):
        s = stage - 1
        ag[s, col] = v.T.astype(jnp.bfloat16)
        own = ag.at[s, col]
        for o in range(1, Z):
            send(own, own, ag_send.at[s, o], ag_recv.at[s, col], {"col": col_partner(2 * o)})
        send(own, own, ag_send.at[s, 0], ag_recv.at[s, col], {"col": peer})

        def add(c, first=False):
            panel = ag[s, c]

            def one(k):
                value = jnp.dot(panel, tile_at(c, k), preferred_element_type=jnp.float32)
                acc[s, k] = value if first else acc[s, k] + value
            each(R, one, unroll)

        add(col, first=True)
        arrive(ag.at[s, peer], ag_recv.at[s, peer])
        add(peer)
        for o in range(1, Z):
            c = col_partner(2 * o)
            block = ag.at[s, c]
            arrive(block, ag_recv.at[s, c])
            send(block, block, ag_send.at[s, Z + o], ag_recv.at[s, c], {"col": peer})
            add(c)
        if first_norm:
            stats_middle(ITERS)
        for o in range(1, Z):
            c = col_partner(2 * o + 1)
            arrive(ag.at[s, c], ag_recv.at[s, c])

        def finish(k):
            value = acc[s, k]
            for o in range(1, Z):
                c = col_partner(2 * o + 1)
                value = value + jnp.dot(ag[s, c], tile_at(c, k), preferred_element_type=jnp.float32)
            acc[s, k] = value

        mixed = scatter(stage, acc.at[s], rs.at[s], finish).T
        product = jnp.where(unlabeled[...] > 0.0, degree[...] * v - mixed, v)
        return product

    x_out[...] = jnp.zeros((B, K), jnp.float32)
    r_out[...] = rhs
    direction[...] = rhs
    stats_start(ITERS, [inner(rhs, rhs)])
    for iteration in range(ITERS):
        product = operator(iteration + 1, direction[...], iteration == 0)
        image[...] = product
        d, r = direction[...], r_out[...]
        if iteration == 0:
            norm = stats_end(ITERS)[0:1]
        last = iteration + 1 == ITERS
        stats_start(
            iteration, [inner(d, product)] + ([] if last else [inner(r, product), inner(product, product)])
        )
        stats_middle(iteration)
        sums = stats_end(iteration)
        alpha = norm / sums[0:1]
        d, i = direction[...], image[...]
        r = r_out[...] - alpha * i
        r_out[...] = r
        x = x_out[...] + alpha * d
        if last:
            x_out[...] = (8.0 * K) * x
        else:
            norm_next = norm - 2.0 * alpha * sums[1:2] + alpha * alpha * sums[2:3]
            direction[...] = r + norm_next / norm * d
            x_out[...] = x
            norm = norm_next
    for cp in sent:
        cp.wait_send()


def solution(mesh):
    R, C = mesh.shape["row"], mesh.shape["col"]

    def shards(tiles, tile_row, tile_col, label_class):
        T, B = tiles.shape[0], tiles.shape[1]
        K = CLASSES
        place = (tile_row % C) * R + tile_col // C
        slot = jnp.arange(R * C, dtype=jnp.int32)
        index = jnp.arange(T, dtype=jnp.int32)
        pos = T - jnp.sum(jnp.where(place[None, :] == slot[:, None], T - index[None, :], 0), axis=1)
        held = T if T == R * C else T + 1
        f32, bf16 = jnp.float32, jnp.bfloat16
        dma = pltpu.SemaphoreType.DMA
        vmem = pl.BlockSpec(memory_space=pltpu.VMEM)
        node = pltpu.VMEM((B, K), f32)
        return pl.pallas_call(
            functools.partial(kernel, R, C),
            out_shape=(jax.ShapeDtypeStruct((B, K), f32), jax.ShapeDtypeStruct((B, K), f32)),
            in_specs=[
                pl.BlockSpec(memory_space=pltpu.SMEM),
                vmem,
                pl.BlockSpec(memory_space=pl.ANY),
            ],
            out_specs=(vmem, vmem),
            scratch_shapes=[
                pltpu.VMEM((held, B, B), bf16),
                pltpu.VMEM((C, 8, B), jnp.int32),
                pltpu.VMEM((C, K + PAD, B), bf16),
                pltpu.VMEM((ITERS, C, K, B), bf16),
                pltpu.VMEM((R, K + DEG, B), f32),
                pltpu.VMEM((ITERS, R, K, B), f32),
                pltpu.VMEM((R - 1, K + DEG, B), f32),
                pltpu.VMEM((ITERS, R - 1, K, B), f32),
                pltpu.VMEM((ITERS + 1, C, 8, K), f32),
                pltpu.VMEM((ITERS + 1, 8, K), f32),
                pltpu.VMEM((ITERS + 1, R, 8, K), f32),
                node, node, node, node,
                dma((PARTS,)),
                dma((C,)), dma((C,)),
                dma((ITERS, C)), dma((ITERS, C)),
                dma((ITERS + 1, C)), dma((ITERS + 1, C)),
                dma((ITERS + 1, R)), dma((ITERS + 1, R)),
                dma((ITERS + 1, R)), dma((ITERS + 1, R)),
            ],
            compiler_params=pltpu.CompilerParams(
                collective_id=0, has_side_effects=True, vmem_limit_bytes=48 * 1024 * 1024
            ),
        )(pos.astype(jnp.int32), label_class.reshape(1, B), tiles)

    placed = (P(("row", "col"), None, None),) + (P(("row", "col")),) * 3
    return jax.shard_map(
        shards,
        mesh=mesh,
        in_specs=placed,
        out_specs=(P(("row", "col"), None), P(("row", "col"), None)),
        check_vma=False,
    )
```

```python
import functools

import jax
import jax.numpy as jnp
from jax import lax
from jax.experimental import pallas as pl
from jax.experimental.pallas import tpu as pltpu
from jax.sharding import PartitionSpec as P

CLASSES = 128
ITERS = 3
PAD = 16
DEG = 8
UNROLL = 32
PARTS = 4


def each(count, body, unroll):
    if unroll:
        for n in range(count):
            body(n)
    else:
        def step(n, carry):
            body(n)
            return carry
        lax.fori_loop(0, count, step, 0)


def flip(index, mask):
    bit = 1
    result = index
    while bit <= mask:
        if mask & bit:
            result = result + bit * (1 - 2 * lax.rem(lax.div(index, bit), 2))
        bit *= 2
    return result


def kernel(
    R, C, pos, label_ref, tiles_hbm, x_out, r_out,
    tiles, lab, ag0, ag, acc0a, acc0b, acc, rs0a, rs0b, rs, st_ag, st_row, st_rs,
    degree, direction, image, residual, answer,
    tile_sem, lab_send, lab_recv, ag_send, ag_recv, st_send, st_recv,
    str_send, str_recv, rs_send, rs_recv,
):
    T, B = tiles_hbm.shape[0], tiles_hbm.shape[1]
    Z = C // 2
    K, H = CLASSES, CLASSES // 2
    unroll = R * C <= UNROLL
    row, col = lax.axis_index("row"), lax.axis_index("col")
    core = lax.rem(col, 2)
    peer = col + 1 - 2 * core
    pow2_z = Z & (Z - 1) == 0
    pow2_r = R & (R - 1) == 0
    assert pow2_z and pow2_r

    def col_partner(m):
        return flip(col, m)

    def row_partner(m):
        return flip(row, m)

    step = -(-T // PARTS)
    tile_copies = []
    for p in range(PARTS):
        lo, hi = p * step, min(T, (p + 1) * step)
        if lo < hi:
            cp = pltpu.make_async_copy(
                tiles_hbm.at[pl.ds(lo, hi - lo)], tiles.at[pl.ds(lo, hi - lo)], tile_sem.at[p]
            )
            cp.start()
            tile_copies.append(cp)
    if tiles.shape[0] > T:
        tiles[T] = jnp.zeros((B, B), jnp.bfloat16)

    barrier = pltpu.get_barrier_semaphore()
    for m in range(1, C):
        pl.semaphore_signal(
            barrier, inc=1, device_id={"col": col_partner(m)}, device_id_type=pl.DeviceIdType.MESH
        )
    for m in range(1, R):
        pl.semaphore_signal(
            barrier, inc=1, device_id={"row": row_partner(m)}, device_id_type=pl.DeviceIdType.MESH
        )
    mine = label_ref[...]
    lab[col] = jnp.broadcast_to(mine, (8, B))
    pl.semaphore_wait(barrier, C - 1 + R - 1)

    sent = []

    def send(src, dst, send_sem, recv_sem, where):
        cp = pltpu.make_async_remote_copy(
            src_ref=src, dst_ref=dst, send_sem=send_sem, recv_sem=recv_sem,
            device_id=where, device_id_type=pl.DeviceIdType.MESH,
        )
        cp.start()
        sent.append(cp)

    def arrive(dst, recv_sem):
        pltpu.make_async_remote_copy(
            src_ref=dst, dst_ref=dst, send_sem=tile_sem.at[0], recv_sem=recv_sem,
            device_id={"col": peer}, device_id_type=pl.DeviceIdType.MESH,
        ).wait_recv()

    def tile_at(source, k):
        return tiles[pos[source * R + k]]

    def scatter_start(t, total, slots, k_body):
        for m in range(R - 1, 0, -1):
            k = row_partner(m)
            k_body(k)
            send(total.at[k], slots.at[m - 1], rs_send.at[t, m], rs_recv.at[t, m], {"row": k})
        k_body(row)

    def scatter_end(t, total, slots):
        result = total[row]
        for m in range(1, R):
            arrive(slots.at[m - 1], rs_recv.at[t, m])
            result = result + slots[m - 1]
        return result

    def inner(a, b):
        product = a * b
        folded = product[:, :K]
        for lane in range(K, B, K):
            folded = folded + product[:, lane : lane + K]
        padded = jnp.concatenate([folded, jnp.zeros((K - H, K), jnp.float32)], axis=0)
        return jnp.sum(padded.T, axis=0, keepdims=True)

    def spread(values):
        square = jnp.broadcast_to(values, (K, K)).T[:H]
        return jnp.concatenate([square] * (B // K), axis=1)

    def stats_start(t, rows):
        st_ag[t, col] = jnp.concatenate(rows + [jnp.zeros((8 - len(rows), K), jnp.float32)], axis=0)
        for m in range(1, C):
            send(st_ag.at[t, col], st_ag.at[t, col], st_send.at[t, m], st_recv.at[t, col],
                 {"col": col_partner(m)})

    def stats_middle(t):
        for m in range(1, C):
            c = col_partner(m)
            arrive(st_ag.at[t, c], st_recv.at[t, c])
        st_row[t] = jnp.sum(st_ag[t], axis=0)
        for m in range(1, R):
            send(st_row.at[t], st_rs.at[t, row], str_send.at[t, m], str_recv.at[t, row],
                 {"row": row_partner(m)})
        st_rs[t, row] = st_row[t]

    def stats_end(t):
        for m in range(1, R):
            k = row_partner(m)
            arrive(st_rs.at[t, k], str_recv.at[t, k])
        return jnp.sum(st_rs[t], axis=0)

    for m in range(1, C):
        send(lab.at[col], lab.at[col], lab_send.at[m], lab_recv.at[col], {"col": col_partner(m)})
    class_axis = lax.broadcasted_iota(jnp.int32, (K, B), 0)
    ones = jnp.ones((PAD, B), jnp.bfloat16)

    def encode(c):
        hot = jnp.where(lab[c][0:1] == class_axis, 1.0, 0.0).astype(jnp.bfloat16)
        ag0[c] = jnp.concatenate([hot[:H], ones, hot[H:]], axis=0)

    encode(col)
    for m in range(1, C):
        c = col_partner(m)
        arrive(lab.at[c], lab_recv.at[c])
        encode(c)
    for cp in tile_copies:
        cp.wait()
    free = jnp.broadcast_to(mine, (H, B)) < 0

    def chain(h):
        lo, rows_in = (0, H + PAD) if h == 0 else (H + PAD, H)
        total, slots = (acc0a, rs0a) if h == 0 else (acc0b, rs0b)
        keep = total.shape[1]

        def first_products(k):
            def one(c, value):
                return value + jnp.dot(
                    ag0[c, lo : lo + rows_in], tile_at(c, k), preferred_element_type=jnp.float32
                )
            value = jnp.zeros((rows_in, B), jnp.float32)
            if unroll:
                for c in range(C):
                    value = one(c, value)
            else:
                value = lax.fori_loop(0, C, one, value)
            total[k] = value[:keep]

        scatter_start(h, total, slots, first_products)
        yield
        value = scatter_end(h, total, slots)
        if h == 0:
            degree[...] = value[H : H + DEG]
        rhs = jnp.where(free, value[:H], 0.0)
        answer[h] = jnp.zeros((H, B), jnp.float32)
        residual[h] = rhs
        direction[h] = rhs
        start = 2 * ITERS + h
        for iteration in range(ITERS):
            s = 2 * iteration + h
            last = iteration + 1 == ITERS
            ag[s, col] = direction[h].astype(jnp.bfloat16)
            own = ag.at[s, col]
            for o in range(1, Z):
                send(own, own, ag_send.at[s, o], ag_recv.at[s, col], {"col": col_partner(2 * o)})
            send(own, own, ag_send.at[s, 0], ag_recv.at[s, col], {"col": peer})
            if iteration == 0:
                stats_start(start, [inner(rhs, rhs)])

            def add(c, first=False):
                panel = ag[s, c]

                def one(k):
                    part = jnp.dot(panel, tile_at(c, k), preferred_element_type=jnp.float32)
                    acc[s, k] = part if first else acc[s, k] + part
                each(R, one, unroll)

            add(col, first=True)
            yield
            arrive(ag.at[s, peer], ag_recv.at[s, peer])
            add(peer)
            for o in range(1, Z):
                c = col_partner(2 * o)
                block = ag.at[s, c]
                arrive(block, ag_recv.at[s, c])
                send(block, block, ag_send.at[s, Z + o], ag_recv.at[s, c], {"col": peer})
                add(c)
            if iteration == 0:
                stats_middle(start)
            yield
            for o in range(1, Z):
                c = col_partner(2 * o + 1)
                arrive(ag.at[s, c], ag_recv.at[s, c])

            def finish(k):
                part = acc[s, k]
                for o in range(1, Z):
                    c = col_partner(2 * o + 1)
                    part = part + jnp.dot(ag[s, c], tile_at(c, k), preferred_element_type=jnp.float32)
                acc[s, k] = part

            scatter_start(2 + s, acc.at[s], rs.at[s], finish)
            yield
            mixed = scatter_end(2 + s, acc.at[s], rs.at[s])
            d, r = direction[h], residual[h]
            i = jnp.where(free, degree[0:1] * d - mixed, d)
            image[h] = i
            stats_start(s, [inner(d, i)] + ([] if last else [inner(r, i), inner(i, i)]))
            yield
            stats_middle(s)
            yield
            if iteration == 0:
                norm = stats_end(start)[0:1]
            sums = stats_end(s)
            alpha = norm / sums[0:1]
            wide = spread(alpha)
            d = direction[h]
            r = residual[h] - wide * image[h]
            x = answer[h] + wide * d
            if last:
                x_out[:, h * H : (h + 1) * H] = ((8.0 * K) * x).T
                r_out[:, h * H : (h + 1) * H] = r.T
            else:
                norm_next = norm - 2.0 * alpha * sums[1:2] + alpha * alpha * sums[2:3]
                direction[h] = r + spread(norm_next / norm) * d
                residual[h] = r
                answer[h] = x
                norm = norm_next

    running = [chain(0), chain(1)]
    while running:
        for one in list(running):
            if next(one, running) is running:
                running.remove(one)
    for cp in sent:
        cp.wait_send()


def solution(mesh):
    R, C = mesh.shape["row"], mesh.shape["col"]

    def shards(tiles, tile_row, tile_col, label_class):
        T, B = tiles.shape[0], tiles.shape[1]
        K, H = CLASSES, CLASSES // 2
        place = (tile_row % C) * R + tile_col // C
        slot = jnp.arange(R * C, dtype=jnp.int32)
        index = jnp.arange(T, dtype=jnp.int32)
        held = T if T == R * C else T + 1
        pos = jnp.max(jnp.where(place[None, :] == slot[:, None], T - index[None, :], T + 1 - held), axis=1)
        pos = T - pos
        f32, bf16 = jnp.float32, jnp.bfloat16
        dma = pltpu.SemaphoreType.DMA
        vmem = pl.BlockSpec(memory_space=pltpu.VMEM)
        node = pltpu.VMEM((2, H, B), f32)
        return pl.pallas_call(
            functools.partial(kernel, R, C),
            out_shape=(jax.ShapeDtypeStruct((B, K), f32), jax.ShapeDtypeStruct((B, K), f32)),
            in_specs=[
                pl.BlockSpec(memory_space=pltpu.SMEM),
                vmem,
                pl.BlockSpec(memory_space=pl.ANY),
            ],
            out_specs=(vmem, vmem),
            scratch_shapes=[
                pltpu.VMEM((held, B, B), bf16),
                pltpu.VMEM((C, 8, B), jnp.int32),
                pltpu.VMEM((C, K + PAD, B), bf16),
                pltpu.VMEM((2 * ITERS, C, H, B), bf16),
                pltpu.VMEM((R, H + DEG, B), f32),
                pltpu.VMEM((R, H, B), f32),
                pltpu.VMEM((2 * ITERS, R, H, B), f32),
                pltpu.VMEM((R - 1, H + DEG, B), f32),
                pltpu.VMEM((R - 1, H, B), f32),
                pltpu.VMEM((2 * ITERS, R - 1, H, B), f32),
                pltpu.VMEM((2 * ITERS + 2, C, 8, K), f32),
                pltpu.VMEM((2 * ITERS + 2, 8, K), f32),
                pltpu.VMEM((2 * ITERS + 2, R, 8, K), f32),
                pltpu.VMEM((DEG, B), f32),
                node, node, node, node,
                dma((PARTS,)),
                dma((C,)), dma((C,)),
                dma((2 * ITERS, C)), dma((2 * ITERS, C)),
                dma((2 * ITERS + 2, C)), dma((2 * ITERS + 2, C)),
                dma((2 * ITERS + 2, R)), dma((2 * ITERS + 2, R)),
                dma((2 * ITERS + 2, R)), dma((2 * ITERS + 2, R)),
            ],
            compiler_params=pltpu.CompilerParams(
                collective_id=0, has_side_effects=True, vmem_limit_bytes=63 * 1024 * 1024
            ),
        )(pos.astype(jnp.int32), label_class.reshape(1, B), tiles)

    placed = (P(("row", "col"), None, None),) + (P(("row", "col")),) * 3
    return jax.shard_map(
        shards,
        mesh=mesh,
        in_specs=placed,
        out_specs=(P(("row", "col"), None), P(("row", "col"), None)),
        check_vma=False,
    )
```
